16 devices in a mesh: tp: 4 (over z, y), dp: 4 (over x, core).
Axes of the slice: x: 2, y: 2, z: 2, core: 2. Of those that a mesh axis runs over, the one named last changes fastest.
Arguments:
- x: bfloat16 [4096, 5120], P(('dp', 'tp'))
- w_gate: bfloat16 [5120, 13824], P('dp', 'tp')
- w_up: bfloat16 [5120, 13824], P('dp', 'tp')
- w_down: bfloat16 [13824, 5120], P('tp', 'dp')
- dy: bfloat16 [4096, 5120], P(('dp', 'tp'))
Outputs:
- output 1: bfloat16 [4096, 5120], P(('dp', 'tp'))
- output 2: bfloat16 [4096, 5120], P(('dp', 'tp'))
- output 3: float32 [5120, 13824], P('dp', 'tp')
- output 4: float32 [5120, 13824], P('dp', 'tp')
- output 5: float32 [13824, 5120], P('tp', 'dp')
All inputs are finite; a program needn't handle non-finite values.
Results may differ from the reference program's by a relative error of at most 0.0012.
Values are sent between devices in bfloat16 or wider.
A program may use at most 1 GiB of HBM per device.

```python
import jax
import jax.numpy as jnp
from jax import lax

ROWS = 4096
D = 5120
FF = 13824


def setup_inputs(seed: int = 0) -> dict:
    ks = jax.random.split(jax.random.key(seed), 5)
    x = jax.random.normal(ks[0], (ROWS, D), jnp.float32)
    w_gate = jax.random.normal(ks[1], (D, FF), jnp.float32) * (D ** -0.5)
    w_up = jax.random.normal(ks[2], (D, FF), jnp.float32) * (D ** -0.5)
    w_down = jax.random.normal(ks[3], (FF, D), jnp.float32) * (1.5 * FF ** -0.5)
    dy = jax.random.normal(ks[4], (ROWS, D), jnp.float32)
    return dict(x=x.astype(jnp.bfloat16), w_gate=w_gate.astype(jnp.bfloat16), w_up=w_up.astype(jnp.bfloat16), w_down=w_down.astype(jnp.bfloat16), dy=dy.astype(jnp.bfloat16))


def reference(x, w_gate, w_up, w_down, dy):
    nb = ROWS // 256
    xs = x.reshape(nb, ROWS // nb, D)
    dys = dy.reshape(nb, ROWS // nb, D)

    def body(carry, inp):
        gw, uw, dw = carry
        xb, dyb = inp
        a = jnp.dot(xb, w_gate, preferred_element_type=jnp.float32)
        b = jnp.dot(xb, w_up, preferred_element_type=jnp.float32)
        sig = jax.nn.sigmoid(a)
        sa = a * sig
        h = (sa * b).astype(jnp.bfloat16)
        y = (xb.astype(jnp.float32) + jnp.dot(h, w_down, preferred_element_type=jnp.float32)).astype(jnp.bfloat16)
        g = jnp.dot(dyb, w_down.T, preferred_element_type=jnp.float32)
        da = (g * b * sig * (1.0 + a * (1.0 - sig))).astype(jnp.bfloat16)
        db = (g * sa).astype(jnp.bfloat16)
        dx = (dyb.astype(jnp.float32) + jnp.dot(da, w_gate.T, preferred_element_type=jnp.float32) + jnp.dot(db, w_up.T, preferred_element_type=jnp.float32)).astype(jnp.bfloat16)
        gw = gw + jnp.dot(xb.T, da, preferred_element_type=jnp.float32)
        uw = uw + jnp.dot(xb.T, db, preferred_element_type=jnp.float32)
        dw = dw + jnp.dot(h.T, dyb, preferred_element_type=jnp.float32)
        return (gw, uw, dw), (y, dx)

    init = (jnp.zeros((D, FF), jnp.float32), jnp.zeros((D, FF), jnp.float32), jnp.zeros((FF, D), jnp.float32))
    (gw, uw, dw), (ys, dxs) = lax.scan(body, init, (xs, dys))
    return ys.reshape(ROWS, D), dxs.reshape(ROWS, D), gw, uw, dw
```

```python
import functools

import jax
import jax.numpy as jnp
from jax import lax
from jax.experimental import pallas as pl
from jax.experimental.pallas import tpu as pltpu
from jax.sharding import PartitionSpec as P


f32 = jnp.float32
bf = jnp.bfloat16
TILE = 256
CHUNK = 1280


def dot(u, v):
    return jnp.dot(u, v, preferred_element_type=f32)


def params():
    return pltpu.CompilerParams(vmem_limit_bytes=60 * 2**20)


def cost(flops, nbytes):
    return pl.CostEstimate(flops=int(flops), bytes_accessed=int(nbytes), transcendentals=0)


def quarters(buf, m, ws):
    dq = ws[0].shape[0]
    acc = dot(buf[m, :, :dq], ws[0][...])
    for k in range(1, 4):
        acc += dot(buf[m, :, k * dq : (k + 1) * dq], ws[k][...])
    return acc


def load(pieces, buf, sems):
    m, n = pl.program_id(0), pl.program_id(1)
    r, w = pieces[0].shape
    copies = []
    for k, p in enumerate(pieces):
        g, row, col = k // 8, k % 8 // 2, k % 2
        dst = buf.at[g, pl.ds(row * r, r), pl.ds(col * w, w)]
        copies.append(pltpu.make_async_copy(p, dst, sems.at[k]))

    @pl.when((m == 0) & (n == 0))
    def _():
        for c in copies:
            c.start()
        for c in copies[:8]:
            c.wait()

    @pl.when((m == 1) & (n == 0))
    def _():
        for c in copies[8:]:
            c.wait()

    return m


def fwd_body(*refs):
    pieces, ws, (a_ref, b_ref, ht_ref), (buf, sems) = refs[:16], refs[16:24], refs[24:27], refs[27:]
    m = load(pieces, buf, sems)
    a = quarters(buf, m, ws[:4])
    b = quarters(buf, m, ws[4:])
    a_ref[...] = a
    b_ref[...] = b
    ht_ref[...] = (a * jax.nn.sigmoid(a) * b).T.astype(bf)


def bwd_body(*refs):
    pieces, ws, (a_ref, b_ref, da_ref, db_ref, dat_ref, dbt_ref), (buf, sems) = refs[:16], refs[16:20], refs[20:26], refs[26:]
    m = load(pieces, buf, sems)
    g = quarters(buf, m, ws)
    a = a_ref[...]
    s = jax.nn.sigmoid(a)
    da = g * b_ref[...] * s * (1.0 + a * (1.0 - s))
    db = g * (a * s)
    da_ref[...] = da.astype(bf)
    db_ref[...] = db.astype(bf)

    @pl.when(m == 0)
    def _():
        dat_ref[...] = da.T.astype(bf)
        dbt_ref[...] = db.T.astype(bf)


def weight_specs(own, c):
    dq = own.shape[0]
    first = c * (CHUNK // TILE)
    whole = pl.BlockSpec((dq, TILE), lambda m, n: (0, first + n))
    piece = pl.BlockSpec((dq, TILE), lambda m, n: (0, n))
    return [whole, whole, piece, piece]


def grouped(body, pieces, ws, wspecs, extra, fc, outs, flops):
    tm = 4 * pieces[0].shape[0]
    d = 2 * pieces[0].shape[1]
    nt = pl.cdiv(fc, TILE)
    specs = {
        "mn": (pl.BlockSpec((tm, TILE), lambda m, n: (m, n)), (2 * tm, fc)),
        "nm": (pl.BlockSpec((TILE, tm), lambda m, n: (n, m)), (fc, 2 * tm)),
        "n0": (pl.BlockSpec((TILE, tm), lambda m, n: (n + m * (nt - 1 - n), 0)), (fc, tm)),
    }
    return pl.pallas_call(
        body,
        grid=(2, nt),
        in_specs=[pl.BlockSpec(memory_space=pl.ANY)] * 16 + wspecs + [specs["mn"][0]] * len(extra),
        out_specs=[specs[k][0] for k, _ in outs],
        out_shape=[jax.ShapeDtypeStruct(specs[k][1], t) for k, t in outs],
        scratch_shapes=[pltpu.VMEM((2, tm, d), bf), pltpu.SemaphoreType.DMA((16,))],
        compiler_params=params(),
        cost_estimate=cost(flops * tm * d * fc, 8e7),
    )(*pieces, *ws, *extra)


def forward(xp, wg, wu, c):
    fc = wg[2].shape[1]
    outs = [("mn", f32), ("mn", f32), ("nm", bf)]
    return grouped(fwd_body, xp, wg + wu, weight_specs(wg[0], c) * 2, [], fc, outs, 8)


def backward(dyp, wd, a, b, c):
    fc = wd[2].shape[1]
    outs = [("mn", bf), ("mn", bf), ("n0", bf), ("n0", bf)]
    return grouped(bwd_body, dyp, wd, weight_specs(wd[0], c), [a, b], fc, outs, 4)


def part_body(axis, terms, nw, nt, groups, has_acc, *refs):
    ws, ts, rest = refs[:nw], refs[nw : nw + nt], refs[nw + nt :]
    no = 2 * groups
    accs = rest[:no] if has_acc else [None] * no
    outs = rest[-no:]
    cols = ts[0].shape[1] // groups
    w = cols // 4
    stay, leave = ((0, 2), (1, 3)) if axis == "y" else ((0, 1), (2, 3))
    for g in range(groups):
        t = None
        for wi, start, ti in terms:
            fc = ts[ti].shape[0]
            u = dot(ws[wi][:, start : start + fc], ts[ti][:, g * cols : (g + 1) * cols])
            t = u if t is None else t + u
        for o, sel in ((2 * g, stay), (2 * g + 1, leave)):
            for n, k in enumerate(sel):
                v = t[:, k * w : (k + 1) * w]
                if has_acc:
                    v = v + accs[o][:, n * w : (n + 1) * w]
                outs[o][:, n * w : (n + 1) * w] = v


def partial_sums(ws, ts, terms, axis, groups, accs=None):
    dq = ws[0].shape[0]
    half = ts[0].shape[1] // groups // 2
    o = pl.BlockSpec((TILE, half), lambda m: (m, 0))
    no = 2 * groups
    n_in = len(ws) + len(ts)
    flops = sum(2 * dq * ts[t[2]].shape[0] * ts[0].shape[1] for t in terms)
    return pl.pallas_call(
        functools.partial(part_body, axis, terms, len(ws), len(ts), groups, accs is not None),
        grid=(dq // TILE,),
        in_specs=[pl.BlockSpec((TILE, w.shape[1]), lambda m: (m, 0)) for w in ws]
        + [pl.BlockSpec(t.shape, lambda m: (0, 0)) for t in ts]
        + ([o] * no if accs else []),
        out_specs=[o] * no,
        out_shape=[jax.ShapeDtypeStruct((dq, half), f32)] * no,
        input_output_aliases={n_in + k: k for k in range(no)} if accs else {},
        compiler_params=params(),
        cost_estimate=cost(flops, 3e7),
        name="partial_sums",
    )(*ws, *ts, *(accs or []))


def dw_body(counts, rows, *refs):
    n = pl.program_id(0)
    fixed, out = refs[:2], refs[-1]
    for c, (lo, hi) in enumerate(counts):
        u, v = refs[2 + 2 * c : 4 + 2 * c]

        @pl.when((n >= lo) & (n < hi))
        def _(u=u, v=v):
            if rows:
                out[...] = dot(u[...], fixed[0][...]) + dot(v[...], fixed[1][...])
            else:
                out[...] = dot(fixed[0][...], u[...]) + dot(fixed[1][...], v[...])


def weight_grad(fixed, streams, rows, full, first, prev=None):
    m = fixed[0].shape[1] if rows else fixed[0].shape[0]
    k = fixed[0].shape[0] if rows else fixed[0].shape[1]
    counts, n = [], 0
    specs = []
    for u, _ in streams:
        nt = pl.cdiv(u.shape[0] if rows else u.shape[1], TILE)

        def index(j, lo=n, nt=nt):
            t = jnp.clip(j - lo, 0, nt - 1)
            return (t, 0) if rows else (0, t)

        specs += [pl.BlockSpec((TILE, k) if rows else (k, TILE), index)] * 2
        counts.append((n, n + nt))
        n += nt
    fspec = pl.BlockSpec(fixed[0].shape, lambda j: (0, 0))
    base = first * (CHUNK // TILE)
    ospec = pl.BlockSpec((TILE, m), lambda j: (base + j, 0)) if rows else pl.BlockSpec((m, TILE), lambda j: (0, base + j))
    n_in = 2 + 2 * len(streams)
    return pl.pallas_call(
        functools.partial(dw_body, counts, rows),
        grid=(n,),
        in_specs=[fspec, fspec] + specs + ([] if prev is None else [pl.BlockSpec(memory_space=pl.ANY)]),
        out_specs=ospec,
        out_shape=jax.ShapeDtypeStruct((full, m) if rows else (m, full), f32),
        input_output_aliases={} if prev is None else {n_in: 0},
        compiler_params=params(),
        cost_estimate=cost(4 * m * k * n * TILE, 5e7),
        name="weight_grad",
    )(*fixed, *[v for p in streams for v in p], *([] if prev is None else [prev]))


def solution(mesh):
    rows = P(("dp", "tp"), None)
    wsp = P("dp", "tp")
    dsp = P("tp", "dp")

    def hop(axis, bit):
        pairs = [(k, k ^ bit) for k in range(mesh.shape[axis])]
        return lambda v: lax.ppermute(v, axis, pairs)

    px, pc = hop("dp", 2), hop("dp", 1)
    py, pz = hop("tp", 1), hop("tp", 2)

    def after(v, *deps):
        return lax.optimization_barrier((v, deps))[0]

    def cross(v):
        return px(v)

    def body(x, w_gate, w_up, w_down, dy):
        i = lax.axis_index("dp")
        dq, fl = w_gate.shape
        starts = list(range(0, fl, CHUNK))
        nc = len(starts)

        def reorder(v):
            return jnp.concatenate([lax.dynamic_slice_in_dim(v, (i ^ k) * dq, dq, 1) for k in range(4)], axis=1)

        def gather(v, dep=None):
            va, vb = v[:, : 2 * dq], v[:, 2 * dq :]
            a_y, b_z, b_y, a_z = py(va), pz(vb), py(vb), pz(va)
            a1, b1 = (a_y, b_z) if dep is None else after((a_y, b_z), *dep)
            a_yz, b_yz = pz(a1), py(b1)
            return [va, vb, a_y, b_y, a_z, b_z, a_yz, b_yz]

        def swap(v):
            return jnp.concatenate([v[:, 2 * dq :], v[:, : 2 * dq]], axis=1)

        piece = lambda w, c: w[:, starts[c] : starts[c] + CHUNK]
        wgx, wux, wdx = [None] * nc, [None] * nc, [None] * nc
        xo, dyo = reorder(x), reorder(dy)
        x_other = swap(cross(xo))
        for c in range(nc):
            if c == nc - 1:
                dy_other = cross(dyo)
            wgx[c] = cross(piece(w_gate, c))
            wux[c] = cross(piece(w_up, c))
        wd_t = w_down.T
        for c in range(nc):
            wdx[c] = cross(piece(wd_t, c))
        wg_s, wu_s, wd_s = pc(w_gate), pc(w_up), pc(wd_t)

        xp = gather(xo) + gather(x_other)
        dyp = gather(after(dyo, *xp[8:]))
        blk = xo.shape[0]
        col = lambda ps, k: jnp.concatenate([p[:, k * dq : (k + 1) * dq] for p in ps[0::2]], axis=0)
        xq, xq_s = col(xp, 0).T, pc(col(xp, 1).T)

        a, b, ht, ht_s, across = [], [], [], [], []
        done = xp
        for c in range(nc):
            gx, ux = after((wgx[c], wux[c]), *done)
            gs, us = pc(gx), pc(ux)
            across.append([(gx, ux), (gs, us)])
            ac, bc, htc = forward(xp, [w_gate, wg_s, gx, gs], [w_up, wu_s, ux, us], c)
            a.append(ac)
            b.append(bc)
            ht.append(htc)
            ht_s.append(pc(htc))
            done = [htc]
            if c == nc - 2:
                terms = [(0, starts[k], k) for k in range(nc - 1)]
                dy_other = swap(after(dy_other, htc))
                yacc = [partial_sums([w], ht, terms, "yz"[q], 2) for q, w in enumerate((wd_t, wd_s))]
                dyp += gather(dy_other, [yacc[0][0], yacc[1][0]])
                dyq, dyq_s = col(dyp, 0), pc(col(dyp, 1))
                done = [yacc[0][0], yacc[1][0]]
        yacc = [partial_sums([w], ht[-1:], [(0, starts[-1], 0)], "yz"[q], 2, yacc[q]) for q, w in enumerate((wd_t, wd_s))]
        done = [yacc[0][0], yacc[1][0]]

        def first_hop(axis, send):
            return (py if axis == "y" else pz)(send)

        def second_hop(axis, keep, r):
            s = keep[:, blk:] + r[:, blk:]
            return keep[:, :blk] + r[:, :blk], (pz if axis == "y" else py)(s)

        order = [(1, 0), (1, 1), (0, 0), (0, 1)]
        y_first = {(g, q): first_hop("yz"[q], yacc[q][2 * g + 1]) for g, q in order}

        da, db, dat, dbt = [], [], [], []
        for c in range(nc):
            dx_ = after(wdx[c], *done)
            grads = backward(dyp, [wd_t, wd_s, dx_, pc(dx_)], a[c], b[c], c)
            for lst, v in zip((da, db, dat, dbt), grads):
                lst.append(v)
            done = [da[c]]
            if c == nc - 2:
                y_first = dict(zip(order, after([y_first[k] for k in order], *done)))
                y_second = {(g, q): second_hop("yz"[q], yacc[q][2 * g], y_first[g, q]) for g, q in order}
        da_s, db_s = [pc(v) for v in da], [pc(v) for v in db]

        dx_keep, dx_first = [], []
        for q in range(4):
            if q < 2:
                ws = ((w_gate, w_up), (wg_s, wu_s))[q]
                terms = [(0, starts[c], c) for c in range(nc)] + [(1, starts[c], nc + c) for c in range(nc)]
            else:
                ws = [across[c][q - 2][0] for c in range(nc)] + [across[c][q - 2][1] for c in range(nc)]
                terms = [(k, 0, k) for k in range(2 * nc)]
            ts = dat + dbt
            if q:
                ts = after(ts, dx_keep[-1])
            keep, send = partial_sums(list(ws), ts, terms, "yzyz"[q], 1)
            dx_keep.append(keep)
            dx_first.append(first_hop("yzyz"[q], send))

        y_second = dict(zip(order, after([y_second[k] for k in order], *dx_keep)))
        part = lambda g: jnp.concatenate([(s + r).T for s, r in (y_second[g, 0], y_second[g, 1])], axis=1)
        y_out = (x_other[:, : 2 * dq].astype(f32) + part(1)).astype(bf)
        y_in = px(y_out)
        y_own = (xo[:, : 2 * dq].astype(f32) + part(0)).astype(bf)
        y = reorder(jnp.concatenate([y_own, y_in], axis=1))

        xq, dyq = after((xq, dyq), *dx_keep)
        dwd = weight_grad((dyq, dyq_s), list(zip(ht, ht_s)), True, fl, 0)
        dwg = weight_grad((xq, xq_s), list(zip(da, da_s)), False, fl, 0)
        dwu = weight_grad((xq, xq_s), list(zip(db, db_s)), False, fl, 0)

        sums = []
        for q in range(4):
            sums.append(second_hop("yzyz"[q], dx_keep[q], dx_first[q]))
        dx = jnp.concatenate([(s + r).T for s, r in sums], axis=1)
        dx = reorder((dyo.astype(f32) + dx).astype(bf))
        return y, dx, dwg, dwu, dwd

    return jax.shard_map(body, mesh=mesh, in_specs=(rows, wsp, wsp, dsp, rows), out_specs=(rows, rows, wsp, wsp, dsp), check_vma=False)
```

```python
import functools

import jax
import jax.numpy as jnp
from jax import lax
from jax.experimental.layout import Layout, with_layout_constraint
from jax.experimental import pallas as pl
from jax.experimental.pallas import tpu as pltpu
from jax.sharding import PartitionSpec as P


f32 = jnp.float32
bf = jnp.bfloat16
TILE = 256
CHUNK = 1280


def dot(u, v):
    return jnp.dot(u, v, preferred_element_type=f32)


def params():
    return pltpu.CompilerParams(vmem_limit_bytes=60 * 2**20)


def cost(flops, nbytes):
    return pl.CostEstimate(flops=int(flops), bytes_accessed=int(nbytes), transcendentals=0)


def load(pieces, buf, sems):
    m, n = pl.program_id(0), pl.program_id(1)
    r = pieces[0].shape[0]
    copies = []
    for k, p in enumerate(pieces):
        copies.append(pltpu.make_async_copy(p, buf.at[k // 4, pl.ds(k % 4 * r, r)], sems.at[k]))

    @pl.when((m == 0) & (n == 0))
    def _():
        for c in copies:
            c.start()
        for c in copies[:4]:
            c.wait()

    @pl.when((m == 1) & (n == 0))
    def _():
        for c in copies[4:]:
            c.wait()

    return m


def pair(buf, m, w0, w1):
    dq = w0.shape[0]
    return dot(buf[m, :, :dq], w0[...]) + dot(buf[m, :, dq:], w1[...])


def near_body(n_out, *refs):
    pieces, ws, outs, (buf, sems) = refs[:8], refs[8 : 8 + 2 * n_out], refs[8 + 2 * n_out : -2], refs[-2:]
    m = load(pieces, buf, sems)
    for k in range(n_out):
        outs[k][...] = pair(buf, m, ws[2 * k], ws[2 * k + 1])


def fwd_body(*refs):
    pieces, ws, (a0, b0, a_ref, b_ref, ht_ref), (buf, sems) = refs[:8], refs[8:12], refs[12:17], refs[17:]
    m = load(pieces, buf, sems)
    a = a0[...] + pair(buf, m, ws[0], ws[1])
    b = b0[...] + pair(buf, m, ws[2], ws[3])
    a_ref[...] = a
    b_ref[...] = b
    ht_ref[...] = (a * jax.nn.sigmoid(a) * b).T.astype(bf)


def bwd_body(*refs):
    pieces, ws, (g0, a_ref, b_ref, da_ref, db_ref, dat_ref, dbt_ref), (buf, sems) = refs[:8], refs[8:10], refs[10:17], refs[17:]
    m = load(pieces, buf, sems)
    g = g0[...] + pair(buf, m, ws[0], ws[1])
    a = a_ref[...]
    s = jax.nn.sigmoid(a)
    da = g * b_ref[...] * s * (1.0 + a * (1.0 - s))
    db = g * (a * s)
    da_ref[...] = da.astype(bf)
    db_ref[...] = db.astype(bf)

    @pl.when(m == 0)
    def _():
        dat_ref[...] = da.T.astype(bf)
        dbt_ref[...] = db.T.astype(bf)


def grouped(body, pieces, ws, first, extra, fc, outs, aliases={}):
    tm = 4 * pieces[0].shape[0]
    d = pieces[0].shape[1]
    dq = ws[0].shape[0]
    nt = pl.cdiv(fc, TILE)
    specs = {
        "mn": (pl.BlockSpec((tm, TILE), lambda m, n: (m, n)), (2 * tm, fc)),
        "nm": (pl.BlockSpec((TILE, tm), lambda m, n: (n, m)), (fc, 2 * tm)),
        "n0": (pl.BlockSpec((TILE, tm), lambda m, n: (n + m * (nt - 1 - n), 0)), (fc, tm)),
    }
    wspec = pl.BlockSpec((dq, TILE), lambda m, n: (0, first + n))
    return pl.pallas_call(
        body,
        grid=(2, nt),
        in_specs=[pl.BlockSpec(memory_space=pltpu.HBM)] * 8 + [wspec] * len(ws) + [specs["mn"][0]] * len(extra),
        out_specs=[specs[k][0] for k, _ in outs],
        out_shape=[jax.ShapeDtypeStruct(specs[k][1], t) for k, t in outs],
        scratch_shapes=[pltpu.VMEM((2, tm, d), bf), pltpu.SemaphoreType.DMA((8,))],
        input_output_aliases=aliases,
        compiler_params=params(),
        cost_estimate=cost(2 * len(ws) * tm * d * fc, 8e7),
    )(*pieces, *ws, *extra)


def near(pieces, ws, c, fc):
    n_out = len(ws) // 2
    return grouped(functools.partial(near_body, n_out), pieces, ws, c * (CHUNK // TILE), [], fc, [("mn", f32)] * n_out)


def forward(pieces, ws, acc):
    fc = ws[0].shape[1]
    outs = [("mn", f32), ("mn", f32), ("nm", bf)]
    return grouped(fwd_body, pieces, ws, 0, acc, fc, outs, {12: 0, 13: 1})


def backward(pieces, ws, extra):
    fc = ws[0].shape[1]
    outs = [("mn", bf), ("mn", bf), ("n0", bf), ("n0", bf)]
    return grouped(bwd_body, pieces, ws, 0, extra, fc, outs)


def part_body(axis, terms, nw, nt, groups, has_acc, *refs):
    ws, ts, rest = refs[:nw], refs[nw : nw + nt], refs[nw + nt :]
    no = 2 * groups
    accs = rest[:no] if has_acc else [None] * no
    outs = rest[-no:]
    cols = ts[0].shape[1] // groups
    w = cols // 4
    stay, leave = ((0, 2), (1, 3)) if axis == "y" else ((0, 1), (2, 3))
    for g in range(groups):
        t = None
        for wi, start, ti in terms:
            fc = ts[ti].shape[0]
            u = dot(ws[wi][:, start : start + fc], ts[ti][:, g * cols : (g + 1) * cols])
            t = u if t is None else t + u
        for o, sel in ((2 * g, stay), (2 * g + 1, leave)):
            for n, k in enumerate(sel):
                v = t[:, k * w : (k + 1) * w]
                if has_acc:
                    v = v + accs[o][:, n * w : (n + 1) * w]
                outs[o][:, n * w : (n + 1) * w] = v


def partial_sums(ws, ts, terms, axis, groups, accs=None):
    dq = ws[0].shape[0]
    half = ts[0].shape[1] // groups // 2
    o = pl.BlockSpec((TILE, half), lambda m: (m, 0))
    no = 2 * groups
    n_in = len(ws) + len(ts)
    flops = sum(2 * dq * ts[t[2]].shape[0] * ts[0].shape[1] for t in terms)
    return pl.pallas_call(
        functools.partial(part_body, axis, terms, len(ws), len(ts), groups, accs is not None),
        grid=(dq // TILE,),
        in_specs=[pl.BlockSpec((TILE, w.shape[1]), lambda m: (m, 0)) for w in ws]
        + [pl.BlockSpec(t.shape, lambda m: (0, 0)) for t in ts]
        + ([o] * no if accs else []),
        out_specs=[o] * no,
        out_shape=[jax.ShapeDtypeStruct((dq, half), f32)] * no,
        input_output_aliases={n_in + k: k for k in range(no)} if accs else {},
        compiler_params=params(),
        cost_estimate=cost(flops, 3e7),
        name="partial_sums",
    )(*ws, *ts, *(accs or []))


def dw_body(counts, rows, *refs):
    n = pl.program_id(0)
    fixed, out = refs[:2], refs[-1]
    for c, (lo, hi) in enumerate(counts):
        u, v = refs[2 + 2 * c : 4 + 2 * c]

        @pl.when((n >= lo) & (n < hi))
        def _(u=u, v=v):
            if rows:
                out[...] = dot(u[...], fixed[0][...]) + dot(v[...], fixed[1][...])
            else:
                out[...] = dot(fixed[0][...], u[...]) + dot(fixed[1][...], v[...])


def weight_grad(fixed, streams, rows, full, first, prev=None):
    m = fixed[0].shape[1] if rows else fixed[0].shape[0]
    k = fixed[0].shape[0] if rows else fixed[0].shape[1]
    counts, n = [], 0
    specs = []
    for u, _ in streams:
        nt = pl.cdiv(u.shape[0] if rows else u.shape[1], TILE)

        def index(j, lo=n, nt=nt):
            t = jnp.clip(j - lo, 0, nt - 1)
            return (t, 0) if rows else (0, t)

        specs += [pl.BlockSpec((TILE, k) if rows else (k, TILE), index)] * 2
        counts.append((n, n + nt))
        n += nt
    fspec = pl.BlockSpec(fixed[0].shape, lambda j: (0, 0))
    base = first * (CHUNK // TILE)
    ospec = pl.BlockSpec((TILE, m), lambda j: (base + j, 0)) if rows else pl.BlockSpec((m, TILE), lambda j: (0, base + j))
    n_in = 2 + 2 * len(streams)
    return pl.pallas_call(
        functools.partial(dw_body, counts, rows),
        grid=(n,),
        in_specs=[fspec, fspec] + specs + ([] if prev is None else [pl.BlockSpec(memory_space=pl.ANY)]),
        out_specs=ospec,
        out_shape=jax.ShapeDtypeStruct((full, m) if rows else (m, full), f32),
        input_output_aliases={} if prev is None else {n_in: 0},
        compiler_params=params(),
        cost_estimate=cost(4 * m * k * n * TILE, 5e7),
        name="weight_grad",
    )(*fixed, *[v for p in streams for v in p], *([] if prev is None else [prev]))


def finish_body(n_sums, natural, *refs):
    base, sums, rest, out = refs[0], refs[1 : 1 + 3 * n_sums], refs[1 + 3 * n_sums : -1], refs[-1]
    dq = sums[0].shape[0]
    i = lax.axis_index("dp") if natural else 0

    def at(k):
        return pl.ds(pl.multiple_of((i ^ k) * dq, 128), dq) if natural else pl.ds(k * dq, dq)

    for k in range(n_sums):
        keep, r1, r2 = sums[3 * k : 3 * k + 3]
        v = (keep[...] + r1[...] + r2[...]).T
        out[:, at(k)] = (base[:, at(k)].astype(f32) + v).astype(bf)
    for k in range(n_sums, n_sums + 2 * len(rest)):
        p = k - n_sums
        out[:, at(k)] = rest[0][:, p * dq : (p + 1) * dq]


def finish(base, sums, rest=(), natural=True):
    blk = base.shape[0]
    dq = sums[0][0].shape[0]
    sspec = pl.BlockSpec((dq, blk), lambda j: (0, 0))
    whole = lambda v: pl.BlockSpec(v.shape, lambda j: (0, 0))
    return pl.pallas_call(
        functools.partial(finish_body, len(sums), natural),
        grid=(1,),
        in_specs=[whole(base)] + [sspec] * (3 * len(sums)) + [whole(v) for v in rest],
        out_specs=whole(base),
        out_shape=jax.ShapeDtypeStruct(base.shape, bf),
        compiler_params=params(),
        cost_estimate=cost(1e8, 2e7),
        name="finish",
    )(base, *[v for t in sums for v in t], *rest)


def solution(mesh):
    rows = P(("dp", "tp"), None)
    wsp = P("dp", "tp")
    dsp = P("tp", "dp")

    def hop(axis, bit):
        pairs = [(k, k ^ bit) for k in range(mesh.shape[axis])]
        return lambda v: lax.ppermute(v, axis, pairs)

    px, pc = hop("dp", 2), hop("dp", 1)
    py, pz = hop("tp", 1), hop("tp", 2)

    def cross(v):
        return px(v)

    def body(x, w_gate, w_up, w_down, dy):
        i = lax.axis_index("dp")
        dq, fl = w_gate.shape
        starts = list(range(0, fl, CHUNK))
        nc = len(starts)

        def reorder(v):
            return jnp.concatenate([lax.dynamic_slice_in_dim(v, (i ^ k) * dq, dq, 1) for k in range(4)], axis=1)

        def gather(v):
            va, vb = v[:, : 2 * dq], v[:, 2 * dq :]
            a_y, b_z, b_y, a_z = py(va), pz(vb), py(vb), pz(va)
            a_yz, b_yz = pz(a_y), py(b_z)
            return [va, vb, a_y, b_y, a_z, b_z, a_yz, b_yz]

        def swap(v):
            return jnp.concatenate([v[:, 2 * dq :], v[:, : 2 * dq]], axis=1)

        piece = lambda w, c: w[:, starts[c] : starts[c] + CHUNK]
        wgx, wux, wdx = [None] * nc, [None] * nc, [None] * nc
        xo, dyo = reorder(x), reorder(dy)
        x_cross, dy_cross = cross(xo), cross(dyo)
        for c in range(nc):
            wgx[c] = cross(piece(w_gate, c))
            wux[c] = cross(piece(w_up, c))
        wd_t = w_down.T
        for c in range(nc):
            wdx[c] = cross(piece(wd_t, c))
        wg_s, wu_s, wd_s = pc(w_gate), pc(w_up), pc(wd_t)
        width = lambda c: wgx[c].shape[1]

        x_other = swap(x_cross)
        xp = gather(xo) + gather(x_other)
        dyp = gather(dyo) + gather(swap(dy_cross))
        blk = xo.shape[0]
        col = lambda ps, k: jnp.concatenate([p[:, k * dq : (k + 1) * dq] for p in ps[0::2]], axis=0)
        row_major = lambda v: with_layout_constraint(v, Layout(major_to_minor=(0, 1)))
        xq, xq_out = row_major(col(xp, 0)).T, row_major(col(xp, 1)).T
        xq_s = pc(xq_out)
        dyq, dyq_s = col(dyp, 0), pc(col(dyp, 1))

        acc = [None] * nc
        xa = xp[0::2]
        for c in range(nc):
            acc[c] = near(xa, [w_gate, wg_s, w_up, wu_s], c, width(c))
        a, b, ht, ht_s, across, g0 = [], [], [], [], [], [None] * nc
        for c in range(nc):
            gx, ux = wgx[c], wux[c]
            gs, us = pc(gx), pc(ux)
            across.append([(gx, ux), (gs, us)])
            ac, bc, htc = forward(xp[1::2], [gx, gs, ux, us], acc[c])
            a.append(ac)
            b.append(bc)
            ht.append(htc)
            ht_s.append(pc(htc))
            if c == 0:
                for k in range(nc):
                    (g0[k],) = near(dyp[0::2], [wd_t, wd_s], k, width(k))
            if c == nc - 2:
                terms = [(0, starts[k], k) for k in range(nc - 1)]
                yacc = [partial_sums([w], ht, terms, "yz"[q], 2) for q, w in enumerate((wd_t, wd_s))]
        yacc = [partial_sums([w], ht[-1:], [(0, starts[-1], 0)], "yz"[q], 2, yacc[q]) for q, w in enumerate((wd_t, wd_s))]

        def first_hop(axis, send):
            return (py if axis == "y" else pz)(send)

        def second_hop(axis, keep, r):
            return (pz if axis == "y" else py)(keep[:, blk:] + r[:, blk:])

        order = [(1, 0), (1, 1), (0, 0), (0, 1)]
        y_first = {(g, q): first_hop("yz"[q], yacc[q][2 * g + 1]) for g, q in order}

        da, db, dat, dbt = [], [], [], []
        for c in range(nc):
            grads = backward(dyp[1::2], [wdx[c], pc(wdx[c])], [g0[c], a[c], b[c]])
            for lst, v in zip((da, db, dat, dbt), grads):
                lst.append(v)
        dwd = weight_grad((dyq, dyq_s), list(zip(ht, ht_s)), True, fl, 0)
        y_second = {(g, q): second_hop("yz"[q], yacc[q][2 * g], y_first[g, q]) for g, q in order}
        da_s, db_s = [pc(v) for v in da], [pc(v) for v in db]

        dx_keep, dx_first = [], []
        for q in range(4):
            if q < 2:
                ws = ((w_gate, w_up), (wg_s, wu_s))[q]
                terms = [(0, starts[c], c) for c in range(nc)] + [(1, starts[c], nc + c) for c in range(nc)]
            else:
                ws = [across[c][q - 2][0] for c in range(nc)] + [across[c][q - 2][1] for c in range(nc)]
                terms = [(k, 0, k) for k in range(2 * nc)]
            keep, send = partial_sums(list(ws), dat + dbt, terms, "yzyz"[q], 1)
            dx_keep.append(keep)
            dx_first.append(first_hop("yzyz"[q], send))

        sums = lambda g: [(yacc[q][2 * g], y_first[g, q], y_second[g, q]) for q in range(2)]
        y_out = finish(x_other[:, : 2 * dq], sums(1), natural=False)
        y_in = px(y_out)

        dwg = weight_grad((xq, xq_s), list(zip(da, da_s)), False, fl, 0)
        dwu = weight_grad((xq, xq_s), list(zip(db, db_s)), False, fl, 0)
        y = finish(x, sums(0), [y_in])

        dx_sums = []
        for q in range(4):
            dx_sums.append((dx_keep[q], dx_first[q], second_hop("yzyz"[q], dx_keep[q], dx_first[q])))
        dx = finish(dy, dx_sums)
        return y, dx, dwg, dwu, dwd

    return jax.shard_map(body, mesh=mesh, in_specs=(rows, wsp, wsp, dsp, rows), out_specs=(rows, rows, wsp, wsp, dsp), check_vma=False)
```

```python
import functools

import jax
import jax.numpy as jnp
from jax import lax
from jax.experimental.layout import Layout, with_layout_constraint
from jax.experimental import pallas as pl
from jax.experimental.pallas import tpu as pltpu
from jax.sharding import PartitionSpec as P


f32 = jnp.float32
bf = jnp.bfloat16
TILE = 256
CHUNK = 1280


def dot(u, v):
    return jnp.dot(u, v, preferred_element_type=f32)


def params():
    return pltpu.CompilerParams(vmem_limit_bytes=60 * 2**20)


def cost(flops, nbytes):
    return pl.CostEstimate(flops=int(flops), bytes_accessed=int(nbytes), transcendentals=0)


def load(pieces, buf, sems):
    m, n = pl.program_id(0), pl.program_id(1)
    r = pieces[0].shape[0]
    copies = []
    for k, p in enumerate(pieces):
        copies.append(pltpu.make_async_copy(p, buf.at[k // 4, pl.ds(k % 4 * r, r)], sems.at[k]))

    @pl.when((m == 0) & (n == 0))
    def _():
        for c in copies:
            c.start()
        for c in copies[:4]:
            c.wait()

    @pl.when((m == 1) & (n == 0))
    def _():
        for c in copies[4:]:
            c.wait()

    return m


def pair(buf, m, w0, w1):
    dq = w0.shape[0]
    return dot(buf[m, :, :dq], w0[...]) + dot(buf[m, :, dq:], w1[...])


def near_body(n_out, *refs):
    pieces, ws, outs, (buf, sems) = refs[:4], refs[4 : 4 + 2 * n_out], refs[-2 - n_out : -2], refs[-2:]
    r = pieces[0].shape[0]
    dq = ws[0].shape[0]
    copies = [pltpu.make_async_copy(p, buf.at[pl.ds(k * r, r)], sems.at[k]) for k, p in enumerate(pieces)]

    @pl.when(pl.program_id(0) == 0)
    def _():
        for c in copies:
            c.start()
        for c in copies:
            c.wait()

    for k in range(n_out):
        outs[k][...] = dot(buf[:, :dq], ws[2 * k][...]) + dot(buf[:, dq:], ws[2 * k + 1][...])


def fwd_body(*refs):
    pieces, ws, (a0, b0, a_ref, b_ref, ht_ref), (buf, sems) = refs[:8], refs[8:12], refs[12:17], refs[17:]
    m = load(pieces, buf, sems)
    a = a0[...] + pair(buf, m, ws[0], ws[1])
    b = b0[...] + pair(buf, m, ws[2], ws[3])
    a_ref[...] = a
    b_ref[...] = b
    ht_ref[...] = (a * jax.nn.sigmoid(a) * b).T.astype(bf)


def bwd_body(*refs):
    pieces, ws, (g0, a_ref, b_ref, da_ref, db_ref, dat_ref, dbt_ref), (buf, sems) = refs[:8], refs[8:10], refs[10:17], refs[17:]
    m = load(pieces, buf, sems)
    g = g0[...] + pair(buf, m, ws[0], ws[1])
    a = a_ref[...]
    s = jax.nn.sigmoid(a)
    da = g * b_ref[...] * s * (1.0 + a * (1.0 - s))
    db = g * (a * s)
    da_ref[...] = da.astype(bf)
    db_ref[...] = db.astype(bf)

    @pl.when(m == 0)
    def _():
        dat_ref[...] = da.T.astype(bf)
        dbt_ref[...] = db.T.astype(bf)


def grouped(body, pieces, ws, first, extra, fc, outs, aliases={}):
    tm = 4 * pieces[0].shape[0]
    d = pieces[0].shape[1]
    dq = ws[0].shape[0]
    nt = pl.cdiv(fc, TILE)
    specs = {
        "mn": (pl.BlockSpec((tm, TILE), lambda m, n: (m, n)), (2 * tm, fc)),
        "nm": (pl.BlockSpec((TILE, tm), lambda m, n: (n, m)), (fc, 2 * tm)),
        "n0": (pl.BlockSpec((TILE, tm), lambda m, n: (n + m * (nt - 1 - n), 0)), (fc, tm)),
    }
    wspec = pl.BlockSpec((dq, TILE), lambda m, n: (0, first + n))
    return pl.pallas_call(
        body,
        grid=(2, nt),
        in_specs=[pl.BlockSpec(memory_space=pltpu.HBM)] * 8 + [wspec] * len(ws) + [specs["mn"][0]] * len(extra),
        out_specs=[specs[k][0] for k, _ in outs],
        out_shape=[jax.ShapeDtypeStruct(specs[k][1], t) for k, t in outs],
        scratch_shapes=[pltpu.VMEM((2, tm, d), bf), pltpu.SemaphoreType.DMA((8,))],
        input_output_aliases=aliases,
        compiler_params=params(),
        cost_estimate=cost(2 * len(ws) * tm * d * fc, 8e7),
    )(*pieces, *ws, *extra)


def near_both_body(*refs):
    pieces, ws, out, (buf, sems) = refs[:8], refs[8:10], refs[10], refs[11:]
    m = load(pieces, buf, sems)
    out[...] = pair(buf, m, ws[0], ws[1])


def near_both(pieces, ws, c, fc):
    return grouped(near_both_body, pieces, ws, c * (CHUNK // TILE), [], fc, [("mn", f32)])


def near(pieces, ws, c, fc, group, prev):
    n_out = len(ws) // 2
    r, d = pieces[0].shape
    dq = ws[0].shape[0]
    first = c * (CHUNK // TILE)
    n_in = 4 + len(ws)
    hbm = pl.BlockSpec(memory_space=pltpu.HBM)
    return pl.pallas_call(
        functools.partial(near_body, n_out),
        grid=(pl.cdiv(fc, TILE),),
        in_specs=[hbm] * 4 + [pl.BlockSpec((dq, TILE), lambda n: (0, first + n))] * len(ws) + [hbm] * len(prev),
        out_specs=[pl.BlockSpec((4 * r, TILE), lambda n: (group, n))] * n_out,
        out_shape=[jax.ShapeDtypeStruct((8 * r, fc), f32)] * n_out,
        scratch_shapes=[pltpu.VMEM((4 * r, d), bf), pltpu.SemaphoreType.DMA((4,))],
        input_output_aliases={n_in + k: k for k in range(len(prev))},
        compiler_params=params(),
        cost_estimate=cost(8 * len(ws) * r * d * fc, 4e7),
        name="near",
    )(*pieces, *ws, *prev)


def forward(pieces, ws, acc):
    fc = ws[0].shape[1]
    outs = [("mn", f32), ("mn", f32), ("nm", bf)]
    return grouped(fwd_body, pieces, ws, 0, acc, fc, outs, {12: 0, 13: 1})


def backward(pieces, ws, extra):
    fc = ws[0].shape[1]
    outs = [("mn", bf), ("mn", bf), ("n0", bf), ("n0", bf)]
    return grouped(bwd_body, pieces, ws, 0, extra, fc, outs)


def part_body(axis, terms, nw, nt, groups, has_acc, *refs):
    ws, ts, rest = refs[:nw], refs[nw : nw + nt], refs[nw + nt :]
    no = 2 * groups
    accs = rest[:no] if has_acc else [None] * no
    outs = rest[-no:]
    cols = ts[0].shape[1] // groups
    w = cols // 4
    stay, leave = ((0, 2), (1, 3)) if axis == "y" else ((0, 1), (2, 3))
    for g in range(groups):
        t = None
        for wi, start, ti in terms:
            fc = ts[ti].shape[0]
            u = dot(ws[wi][:, start : start + fc], ts[ti][:, g * cols : (g + 1) * cols])
            t = u if t is None else t + u
        for o, sel in ((2 * g, stay), (2 * g + 1, leave)):
            for n, k in enumerate(sel):
                v = t[:, k * w : (k + 1) * w]
                if has_acc:
                    v = v + accs[o][:, n * w : (n + 1) * w]
                outs[o][:, n * w : (n + 1) * w] = v


def partial_sums(ws, ts, terms, axis, groups, accs=None):
    dq = ws[0].shape[0]
    half = ts[0].shape[1] // groups // 2
    o = pl.BlockSpec((TILE, half), lambda m: (m, 0))
    no = 2 * groups
    n_in = len(ws) + len(ts)
    flops = sum(2 * dq * ts[t[2]].shape[0] * ts[0].shape[1] for t in terms)
    return pl.pallas_call(
        functools.partial(part_body, axis, terms, len(ws), len(ts), groups, accs is not None),
        grid=(dq // TILE,),
        in_specs=[pl.BlockSpec((TILE, w.shape[1]), lambda m: (m, 0)) for w in ws]
        + [pl.BlockSpec(t.shape, lambda m: (0, 0)) for t in ts]
        + ([o] * no if accs else []),
        out_specs=[o] * no,
        out_shape=[jax.ShapeDtypeStruct((dq, half), f32)] * no,
        input_output_aliases={n_in + k: k for k in range(no)} if accs else {},
        compiler_params=params(),
        cost_estimate=cost(flops, 3e7),
        name="partial_sums",
    )(*ws, *ts, *(accs or []))


def dw_body(counts, rows, *refs):
    n = pl.program_id(0)
    fixed, out = refs[:2], refs[-1]
    for c, (lo, hi) in enumerate(counts):
        u, v = refs[2 + 2 * c : 4 + 2 * c]

        @pl.when((n >= lo) & (n < hi))
        def _(u=u, v=v):
            if rows:
                out[...] = dot(u[...], fixed[0][...]) + dot(v[...], fixed[1][...])
            else:
                out[...] = dot(fixed[0][...], u[...]) + dot(fixed[1][...], v[...])


def weight_grad(fixed, streams, rows, full, first, prev=None):
    m = fixed[0].shape[1] if rows else fixed[0].shape[0]
    k = fixed[0].shape[0] if rows else fixed[0].shape[1]
    counts, n = [], 0
    specs = []
    for u, _ in streams:
        nt = pl.cdiv(u.shape[0] if rows else u.shape[1], TILE)

        def index(j, lo=n, nt=nt):
            t = jnp.clip(j - lo, 0, nt - 1)
            return (t, 0) if rows else (0, t)

        specs += [pl.BlockSpec((TILE, k) if rows else (k, TILE), index)] * 2
        counts.append((n, n + nt))
        n += nt
    fspec = pl.BlockSpec(fixed[0].shape, lambda j: (0, 0))
    base = first * (CHUNK // TILE)
    ospec = pl.BlockSpec((TILE, m), lambda j: (base + j, 0)) if rows else pl.BlockSpec((m, TILE), lambda j: (0, base + j))
    n_in = 2 + 2 * len(streams)
    return pl.pallas_call(
        functools.partial(dw_body, counts, rows),
        grid=(n,),
        in_specs=[fspec, fspec] + specs + ([] if prev is None else [pl.BlockSpec(memory_space=pl.ANY)]),
        out_specs=ospec,
        out_shape=jax.ShapeDtypeStruct((full, m) if rows else (m, full), f32),
        input_output_aliases={} if prev is None else {n_in: 0},
        compiler_params=params(),
        cost_estimate=cost(4 * m * k * n * TILE, 5e7),
        name="weight_grad",
    )(*fixed, *[v for p in streams for v in p], *([] if prev is None else [prev]))


def finish_body(n_sums, natural, *refs):
    base, sums, rest, out = refs[0], refs[1 : 1 + 3 * n_sums], refs[1 + 3 * n_sums : -1], refs[-1]
    dq = sums[0].shape[0]
    i = lax.axis_index("dp") if natural else 0

    def at(k):
        return pl.ds(pl.multiple_of((i ^ k) * dq, 128), dq) if natural else pl.ds(k * dq, dq)

    for k in range(n_sums):
        keep, r1, r2 = sums[3 * k : 3 * k + 3]
        v = (keep[...] + r1[...] + r2[...]).T
        out[:, at(k)] = (base[:, at(k)].astype(f32) + v).astype(bf)
    for k in range(n_sums, n_sums + 2 * len(rest)):
        p = k - n_sums
        out[:, at(k)] = rest[0][:, p * dq : (p + 1) * dq]


def finish(base, sums, rest=(), natural=True):
    blk = base.shape[0]
    dq = sums[0][0].shape[0]
    sspec = pl.BlockSpec((dq, blk), lambda j: (0, 0))
    whole = lambda v: pl.BlockSpec(v.shape, lambda j: (0, 0))
    return pl.pallas_call(
        functools.partial(finish_body, len(sums), natural),
        grid=(1,),
        in_specs=[whole(base)] + [sspec] * (3 * len(sums)) + [whole(v) for v in rest],
        out_specs=whole(base),
        out_shape=jax.ShapeDtypeStruct(base.shape, bf),
        compiler_params=params(),
        cost_estimate=cost(1e8, 2e7),
        name="finish",
    )(base, *[v for t in sums for v in t], *rest)


def solution(mesh):
    rows = P(("dp", "tp"), None)
    wsp = P("dp", "tp")
    dsp = P("tp", "dp")

    def hop(axis, bit):
        pairs = [(k, k ^ bit) for k in range(mesh.shape[axis])]
        return lambda v: lax.ppermute(v, axis, pairs)

    px, pc = hop("dp", 2), hop("dp", 1)
    py, pz = hop("tp", 1), hop("tp", 2)

    def cross(v):
        return px(v)

    def body(x, w_gate, w_up, w_down, dy):
        i = lax.axis_index("dp")
        dq, fl = w_gate.shape
        starts = list(range(0, fl, CHUNK))
        nc = len(starts)

        def reorder(v):
            return jnp.concatenate([lax.dynamic_slice_in_dim(v, (i ^ k) * dq, dq, 1) for k in range(4)], axis=1)

        def gather(v):
            va, vb = v[:, : 2 * dq], v[:, 2 * dq :]
            a_y, b_z, b_y, a_z = py(va), pz(vb), py(vb), pz(va)
            a_yz, b_yz = pz(a_y), py(b_z)
            return [va, vb, a_y, b_y, a_z, b_z, a_yz, b_yz]

        def swap(v):
            return jnp.concatenate([v[:, 2 * dq :], v[:, : 2 * dq]], axis=1)

        piece = lambda w, c: w[:, starts[c] : starts[c] + CHUNK]
        wgx, wux, wdx = [None] * nc, [None] * nc, [None] * nc
        xo, dyo = reorder(x), reorder(dy)
        x_cross, dy_cross = cross(xo), cross(dyo)
        for c in range(nc):
            wgx[c] = cross(piece(w_gate, c))
            wux[c] = cross(piece(w_up, c))
        wd_t = w_down.T
        for c in range(nc):
            wdx[c] = cross(piece(wd_t, c))
        wg_s, wu_s, wd_s = pc(w_gate), pc(w_up), pc(wd_t)
        width = lambda c: wgx[c].shape[1]

        x_other = swap(x_cross)
        xp = gather(xo) + gather(x_other)
        dyp = gather(dyo) + gather(swap(dy_cross))
        blk = xo.shape[0]
        col = lambda ps, k: jnp.concatenate([p[:, k * dq : (k + 1) * dq] for p in ps[0::2]], axis=0)
        row_major = lambda v: with_layout_constraint(v, Layout(major_to_minor=(0, 1)))
        xq, xq_out = row_major(col(xp, 0)).T, row_major(col(xp, 1)).T
        xq_s = pc(xq_out)
        dyq, dyq_s = col(dyp, 0), pc(col(dyp, 1))

        acc = [[]] * nc
        for g in range(2):
            for c in range(nc):
                acc[c] = near(xp[8 * g : 8 * g + 8 : 2], [w_gate, wg_s, w_up, wu_s], c, width(c), g, acc[c])
        a, b, ht, ht_s, across, g0 = [], [], [], [], [], [[]] * nc
        dwd = None
        for c in range(nc):
            gx, ux = wgx[c], wux[c]
            gs, us = pc(gx), pc(ux)
            across.append([(gx, ux), (gs, us)])
            ac, bc, htc = forward(xp[1::2], [gx, gs, ux, us], acc[c])
            a.append(ac)
            b.append(bc)
            ht.append(htc)
            ht_s.append(pc(htc))
            dwd = weight_grad((dyq, dyq_s), [(htc, ht_s[c])], True, fl, c, dwd)
            if c == 0:
                for k in range(nc):
                    g0[k] = near_both(dyp[0::2], [wd_t, wd_s], k, width(k))
            if c == nc - 2:
                terms = [(0, starts[k], k) for k in range(nc - 1)]
                yacc = [partial_sums([w], ht, terms, "yz"[q], 2) for q, w in enumerate((wd_t, wd_s))]
        yacc = [partial_sums([w], ht[-1:], [(0, starts[-1], 0)], "yz"[q], 2, yacc[q]) for q, w in enumerate((wd_t, wd_s))]

        def first_hop(axis, send):
            return (py if axis == "y" else pz)(send)

        def second_hop(axis, keep, r):
            return (pz if axis == "y" else py)(keep[:, blk:] + r[:, blk:])

        order = [(1, 0), (1, 1), (0, 0), (0, 1)]
        y_first = {(g, q): first_hop("yz"[q], yacc[q][2 * g + 1]) for g, q in order}

        da, db, dat, dbt = [], [], [], []
        for c in range(nc):
            grads = backward(dyp[1::2], [wdx[c], pc(wdx[c])], [*g0[c], a[c], b[c]])
            for lst, v in zip((da, db, dat, dbt), grads):
                lst.append(v)
        y_second = {(g, q): second_hop("yz"[q], yacc[q][2 * g], y_first[g, q]) for g, q in order}
        da_s, db_s = [pc(v) for v in da], [pc(v) for v in db]

        dx_keep, dx_first = [], []
        for q in range(4):
            if q < 2:
                ws = ((w_gate, w_up), (wg_s, wu_s))[q]
                terms = [(0, starts[c], c) for c in range(nc)] + [(1, starts[c], nc + c) for c in range(nc)]
            else:
                ws = [across[c][q - 2][0] for c in range(nc)] + [across[c][q - 2][1] for c in range(nc)]
                terms = [(k, 0, k) for k in range(2 * nc)]
            keep, send = partial_sums(list(ws), dat + dbt, terms, "yzyz"[q], 1)
            dx_keep.append(keep)
            dx_first.append(first_hop("yzyz"[q], send))

        sums = lambda g: [(yacc[q][2 * g], y_first[g, q], y_second[g, q]) for q in range(2)]
        y_out = finish(x_other[:, : 2 * dq], sums(1), natural=False)
        y_in = px(y_out)

        dwg = weight_grad((xq, xq_s), list(zip(da, da_s)), False, fl, 0)
        dwu = weight_grad((xq, xq_s), list(zip(db, db_s)), False, fl, 0)
        y = finish(x, sums(0), [y_in])

        dx_sums = []
        for q in range(4):
            dx_sums.append((dx_keep[q], dx_first[q], second_hop("yzyz"[q], dx_keep[q], dx_first[q])))
        dx = finish(dy, dx_sums)
        return y, dx, dwg, dwu, dwd

    return jax.shard_map(body, mesh=mesh, in_specs=(rows, wsp, wsp, dsp, rows), out_specs=(rows, rows, wsp, wsp, dsp), check_vma=False)
```
